32 devices in a mesh: dp: 4 (over y, x), vocab: 8 (over z, core).
Axes of the slice: x: 2, y: 2, z: 4, core: 2. Of those that a mesh axis runs over, the one named last changes fastest.
Arguments:
- hidden: bfloat16 [256, 3072], P(('dp', 'vocab')), parts along dimension 0, may hold values from -60 to 60
- weight: bfloat16 [3072, 8192], P(None, 'vocab'), may hold values from -0.32421875 to 0.32421875
- targets: int32 [256], P('dp'), parts along dimension 0, may hold values from 0 to 8191
Outputs:
- loss: float32 [4], P('dp'), parts along dimension 0
- d_hidden: bfloat16 [256, 3072], P(('dp', 'vocab')), parts along dimension 0
- d_weight: bfloat16 [12288, 8192], P('dp', 'vocab'), parts along dimension 0
The draws below stay inside these ranges and needn't reach their ends.
There are 4 independent parts, one for each index of `dp`. The reference program is written for one: setup_inputs(seed, part) draws one part's arguments, and reference() takes and returns one part's arrays. A program takes and returns all parts, laid end to end along the dimension named above; an argument that names none is the same for every part. Nothing has to cross between parts.
All inputs are finite; a program needn't handle non-finite values.
Results may differ from the reference program's by a relative error of at most 0.0035.
Values may be sent and summed in bfloat16 or wider, within the bound.
A program may use at most 64 MiB of HBM per device.

```python
import jax
import jax.numpy as jnp
from jax import lax

D = 3072
TOKENS = 64
VOCAB = 8192


def draw_hidden(key, part):
    first = jax.random.fold_in(jax.random.fold_in(key, 17), 0)
    values = jax.random.normal(first, (TOKENS, D), jnp.float32)
    return jnp.clip(values, -60.0, 60.0).astype(jnp.bfloat16)


def touch_ends(result, own_key, low, top_value):
    place = [jax.random.randint(jax.random.fold_in(own_key, axis), (), 0, length) for axis, length in enumerate(result.shape)]
    main_axis = result.shape.index(max(result.shape))
    neighbour = place[:main_axis] + [(place[main_axis] + 1) % result.shape[main_axis]] + place[main_axis + 1:]
    return result.at[tuple(place)].set(low).at[tuple(neighbour)].set(top_value)


def levels(key, dims, shards, least, high):
    level = 1.0
    for axis_at, parts in shards:
        steps = jax.random.uniform(jax.random.fold_in(jax.random.fold_in(key, 6), axis_at), (parts,), jnp.float32, least / len(shards), high / len(shards))
        level = level * jnp.repeat(jnp.exp(steps), dims[axis_at] // parts).reshape((-1,) + (1,) * (len(dims) - 1 - axis_at))
    return level


def noise(rng, extent, width, most, shards=(), kind=jnp.bfloat16):
    drawn = width * jax.random.normal(rng, extent, jnp.float32)
    if shards:
        drawn = drawn * levels(rng, extent, shards, -0.22, 0.18)
    return jnp.clip(drawn, -most, most).astype(kind)


def setup_inputs(seed: int = 0, part: int = 0) -> dict:
    key_list = jax.random.split(jax.random.key(seed), 4)
    part_keys = jax.random.split(jax.random.fold_in(key_list[3], part), 4)
    hidden = draw_hidden(jax.random.fold_in(jax.random.fold_in(key_list[3], part), 71), part)
    weight = noise(key_list[1], (D, VOCAB), (3 / D ** 0.5), 0.32421875, ((1, 8),))
    targets = touch_ends(jax.random.randint(part_keys[2], (TOKENS,), 0, VOCAB), jax.random.fold_in(part_keys[2], 1), 0, VOCAB - 1).astype(jnp.int32)
    return dict(hidden=hidden, weight=weight, targets=targets)


def reference(hidden, weight, targets):
    logits = jnp.dot(hidden, weight, preferred_element_type=jnp.float32)
    top = jnp.max(logits, axis=1)
    expo = jnp.exp(logits - top[:, None])
    total = jnp.sum(expo, axis=1)
    columns = lax.broadcasted_iota(jnp.int32, logits.shape, 1)
    hits = columns == targets.astype(jnp.int32)[:, None]
    picked = jnp.sum(jnp.where(hits, logits, jnp.zeros_like(logits)), axis=1)
    loss = jnp.mean(top + jnp.log(total) - picked).reshape(1)
    grad_logits = (expo / total[:, None] - hits.astype(logits.dtype)).astype(jnp.bfloat16)
    d_hidden = lax.dot_general(grad_logits, weight, (((1,), (1,)), ((), ())), preferred_element_type=jnp.float32).astype(jnp.bfloat16)
    d_weight = lax.dot_general(hidden, grad_logits, (((0,), (0,)), ((), ())), preferred_element_type=jnp.float32).astype(jnp.bfloat16)
    return loss, d_hidden, d_weight
```

```python
import functools

import jax
import jax.numpy as jnp
from jax import lax
from jax.experimental import pallas as pl
from jax.experimental.pallas import tpu as pltpu
from jax.sharding import PartitionSpec as P

MESH = pl.DeviceIdType.MESH
F32 = jnp.float32
BF16 = jnp.bfloat16


def split(length, most, unit):
    for parts in range(most, 0, -1):
        if length % (parts * unit) == 0:
            return parts
    return 1


def remote(src, dst, send, recv, device):
    return pltpu.make_async_remote_copy(
        src_ref=src, dst_ref=dst, send_sem=send, recv_sem=recv, device_id={"vocab": device}, device_id_type=MESH
    )


def loss_kernel(
    n, h_ref, w_hbm, t_ref, hid_ref, g_ref, dh_ref, loss_ref,
    w_v, slots, e_v, stats, part, xbuf, outb, rbuf,
    w_sem, ag_send, fw_send, ag_recv, st_send, st_recv, x_send, x_recv, rs_send, rs_recv,
):
    me = lax.axis_index("vocab")
    chips = n // 2
    chip, core = me // 2, me % 2
    partner = chip * 2 + (1 - core)
    rows, depth = h_ref.shape
    tokens, width = e_v.shape
    pieces, span = slots.shape[0], slots.shape[3]
    parts, wide = part.shape[0], part.shape[4]

    def other(k):
        return lax.rem(chip + k, chips)

    loads = [
        pltpu.make_async_copy(w_hbm.at[pl.ds(a * span, span), :], w_v.at[pl.ds(a * span, span), :], w_sem.at[a])
        for a in range(pieces)
    ]
    for load in loads:
        load.start()

    barrier = pltpu.get_barrier_semaphore()
    for k in range(1, n):
        pl.semaphore_signal(barrier, inc=1, device_id={"vocab": lax.rem(me + k, n)}, device_id_type=MESH)
    for a in range(pieces):
        slots[a, me] = h_ref[:, a * span:(a + 1) * span]
    pl.semaphore_wait(barrier, n - 1)

    sends = []
    for a in range(pieces):
        own = h_ref.at[:, pl.ds(a * span, span)]
        for k in range(chips):
            target = partner if k == 0 else other(k) * 2 + core
            copy = remote(own, slots.at[a, me], ag_send.at[a, k], ag_recv.at[a, me], target)
            copy.start()
            sends.append(copy)

    for a in range(pieces):
        for k in range(1, chips):
            source = other(k) * 2 + core
            copy = remote(slots.at[a, source], slots.at[a, source], fw_send.at[a, k], ag_recv.at[a, source], partner)
            copy.wait_recv()
            copy.start()
            sends.append(copy)
        for k in range(chips):
            source = other(k) * 2 + (1 - core)
            remote(slots.at[a, source], slots.at[a, source], fw_send.at[a, k], ag_recv.at[a, source], partner).wait_recv()
        for z in range(chips):
            both = jnp.concatenate([slots[a, 2 * z].astype(F32), slots[a, 2 * z + 1].astype(F32)], axis=0)
            hid_ref[2 * rows * z:2 * rows * (z + 1), a * span:(a + 1) * span] = both.astype(BF16)
        loads[a].wait()
        term = jnp.dot(
            hid_ref[:, a * span:(a + 1) * span], w_v[a * span:(a + 1) * span, :], preferred_element_type=F32
        )
        if a == 0:
            e_v[...] = term
        else:
            e_v[...] += term

    logits = e_v[...]
    target = jnp.transpose(jnp.broadcast_to(t_ref[...].astype(F32), (128, tokens)))[:, 0:1]
    columns = (me * width + lax.broadcasted_iota(jnp.int32, (tokens, width), 1)).astype(F32)
    hits = columns == target
    local_top = jnp.max(logits, axis=1, keepdims=True)
    expo = jnp.exp(logits - local_top)
    local_total = jnp.sum(expo, axis=1, keepdims=True)
    local_picked = jnp.sum(jnp.where(hits, logits, 0.0), axis=1, keepdims=True)
    e_v[...] = expo
    lane = lax.broadcasted_iota(jnp.int32, (tokens, 128), 1)
    packed = jnp.where(lane == 0, local_top, jnp.where(lane == 1, local_total, local_picked))
    stats[me] = jnp.transpose(packed)[0:8, :]
    for k in range(1, n):
        copy = remote(stats.at[me], stats.at[me], st_send.at[k], st_recv.at[me], lax.rem(me + k, n))
        copy.start()
        sends.append(copy)
    for k in range(1, n):
        source = lax.rem(me + k, n)
        remote(stats.at[source], stats.at[source], st_send.at[k], st_recv.at[source], source).wait_recv()

    top = stats[0, 0:1, :]
    for k in range(1, n):
        top = jnp.maximum(top, stats[k, 0:1, :])
    total = jnp.zeros_like(top)
    picked = jnp.zeros_like(top)
    for k in range(n):
        total += stats[k, 1:2, :] * jnp.exp(stats[k, 0:1, :] - top)
        picked += stats[k, 2:3, :]
    loss_ref[...] = jnp.sum(top + jnp.log(total) - picked, axis=1, keepdims=True) / tokens

    sub = lax.broadcasted_iota(jnp.int32, (128, tokens), 0)
    turned = jnp.transpose(jnp.where(sub == 0, top, total))
    factor = jnp.exp(local_top - turned[:, 0:1]) / turned[:, 1:2]
    grad = (e_v[...] * factor - hits.astype(F32)).astype(BF16)
    g_ref[...] = grad

    def pair_copy(j):
        return remote(part.at[j, 1 - core], xbuf.at[j], x_send.at[j], x_recv.at[j], partner)

    def group_copy(j, k):
        return remote(outb.at[j, other(k)], rbuf.at[j, chip], rs_send.at[j, k], rs_recv.at[j, chip], other(k) * 2 + core)

    def pass_on(j):
        pair_copy(j).wait_recv()
        for z in range(chips):
            outb[j, z] = (part[j, core, z] + xbuf[j, z]).astype(BF16)
        for k in range(1, chips):
            copy = group_copy(j, k)
            copy.start()
            sends.append(copy)

    for j in range(parts):
        term = lax.dot_general(
            g_ref[...], w_v[j * wide:(j + 1) * wide, :], (((1,), (1,)), ((), ())), preferred_element_type=F32
        )
        for z in range(chips):
            for half in range(2):
                at = (2 * z + half) * rows
                part[j, half, z] = term[at:at + rows, :]
        copy = pair_copy(j)
        copy.start()
        sends.append(copy)
        if j > 0:
            pass_on(j - 1)
    pass_on(parts - 1)

    for j in range(parts):
        summed = part[j, core, chip] + xbuf[j, chip]
        for k in range(1, chips):
            source = other(k)
            remote(rbuf.at[j, source], rbuf.at[j, source], rs_send.at[j, k], rs_recv.at[j, source], source * 2 + core).wait_recv()
            summed += rbuf[j, source].astype(F32)
        dh_ref[:, j * wide:(j + 1) * wide] = summed.astype(BF16)

    for copy in sends:
        copy.wait_send()


def weight_kernel(hid_ref, g_ref, out_ref):
    out_ref[...] = lax.dot_general(
        hid_ref[...], g_ref[...], (((0,), (0,)), ((), ())), preferred_element_type=F32
    ).astype(BF16)


def body(n, hidden, weight, targets):
    rows, depth = hidden.shape
    width = weight.shape[1]
    tokens = rows * n
    chips = n // 2
    pieces = split(depth, 2, 256)
    parts = split(depth, 4, 256)
    span, wide = depth // pieces, depth // parts
    vmem = pl.BlockSpec(memory_space=pltpu.VMEM)
    dma = pltpu.SemaphoreType.DMA
    hid, grad, d_hidden, loss = pl.pallas_call(
        functools.partial(loss_kernel, n),
        out_shape=(
            jax.ShapeDtypeStruct((tokens, depth), BF16),
            jax.ShapeDtypeStruct((tokens, width), BF16),
            jax.ShapeDtypeStruct((rows, depth), BF16),
            jax.ShapeDtypeStruct((1, 1), F32),
        ),
        in_specs=[vmem, pl.BlockSpec(memory_space=pl.ANY), vmem],
        out_specs=(vmem, vmem, vmem, vmem),
        scratch_shapes=[
            pltpu.VMEM((depth, width), BF16),
            pltpu.VMEM((pieces, n, rows, span), BF16),
            pltpu.VMEM((tokens, width), F32),
            pltpu.VMEM((n, 8, tokens), F32),
            pltpu.VMEM((parts, 2, chips, rows, wide), F32),
            pltpu.VMEM((parts, chips, rows, wide), F32),
            pltpu.VMEM((parts, chips, rows, wide), BF16),
            pltpu.VMEM((parts, chips, rows, wide), BF16),
            dma((pieces,)),
            dma((pieces, chips)),
            dma((pieces, chips)),
            dma((pieces, n)),
            dma((n,)),
            dma((n,)),
            dma((parts,)),
            dma((parts,)),
            dma((parts, chips)),
            dma((parts, chips)),
        ],
        compiler_params=pltpu.CompilerParams(
            collective_id=0, has_side_effects=True, vmem_limit_bytes=50 * 1024 * 1024
        ),
    )(hidden, weight, targets.reshape(1, tokens))
    block = depth // split(depth, 6, 256)
    d_weight = pl.pallas_call(
        weight_kernel,
        grid=(depth // block,),
        out_shape=jax.ShapeDtypeStruct((depth, width), BF16),
        in_specs=[
            pl.BlockSpec((tokens, block), lambda i: (0, i)),
            pl.BlockSpec((tokens, width), lambda i: (0, 0)),
        ],
        out_specs=pl.BlockSpec((block, width), lambda i: (i, 0)),
    )(hid, grad)
    return loss.reshape(1), d_hidden, d_weight


def solution(mesh):
    placed = (P(("dp", "vocab"), None), P(None, "vocab"), P("dp"))
    return jax.shard_map(
        functools.partial(body, mesh.shape["vocab"]),
        mesh=mesh,
        in_specs=placed,
        out_specs=(P("dp"), P(("dp", "vocab"), None), P("dp", "vocab")),
        check_vma=False,
    )
```

```python
import functools

import jax
import jax.numpy as jnp
from jax import lax
from jax.experimental import pallas as pl
from jax.experimental.pallas import tpu as pltpu
from jax.sharding import PartitionSpec as P

MESH = pl.DeviceIdType.MESH
F32 = jnp.float32
BF16 = jnp.bfloat16


def split(length, most, unit):
    for parts in range(most, 0, -1):
        if length % (parts * unit) == 0:
            return parts
    return 1


def remote(src, dst, send, recv, device):
    return pltpu.make_async_remote_copy(
        src_ref=src, dst_ref=dst, send_sem=send, recv_sem=recv, device_id={"vocab": device}, device_id_type=MESH
    )


def loss_kernel(
    n, h_hbm, w_hbm, t_hbm, dw_ref, dh_ref, loss_ref,
    h_ref, t_ref, hid_ref, turned_ref, g_ref, w_v, slots, e_v, stats, part, xbuf, outb, rbuf,
    in_sem, w_sem, ag_send, fw_send, ag_recv, st_send, st_recv, x_send, x_recv, rs_send, rs_recv,
):
    me = lax.axis_index("vocab")
    chips = n // 2
    chip, core = me // 2, me % 2
    partner = chip * 2 + (1 - core)
    rows, depth = h_ref.shape
    tokens, width = e_v.shape
    pieces, span = slots.shape[0], slots.shape[3]
    parts, wide = part.shape[0], part.shape[4]
    blocks = split(depth, 6, 256)
    tall = depth // blocks

    above = chips - 1 - chip

    def other(k):
        up = (above - k + chips) // chips
        return up * (chips - k) + (1 - up) * (k - 1 - above)

    takes = [pltpu.make_async_copy(h_hbm, h_ref, in_sem.at[0]), pltpu.make_async_copy(t_hbm, t_ref, in_sem.at[1])]
    for take in takes:
        take.start()
    loads = [
        pltpu.make_async_copy(w_hbm.at[pl.ds(a * span, span), :], w_v.at[pl.ds(a * span, span), :], w_sem.at[a])
        for a in range(pieces)
    ]
    for load in loads:
        load.start()

    barrier = pltpu.get_barrier_semaphore()
    for k in range(1, n):
        pl.semaphore_signal(barrier, inc=1, device_id={"vocab": lax.rem(me + k, n)}, device_id_type=MESH)
    for take in takes:
        take.wait()
    for a in range(pieces):
        slots[a, me] = h_ref[:, a * span:(a + 1) * span]
    pl.semaphore_wait(barrier, n - 1)

    sends = []
    for a in range(pieces):
        own = h_ref.at[:, pl.ds(a * span, span)]
        for k in range(chips):
            target = partner if k == 0 else other(k) * 2 + core
            copy = remote(own, slots.at[a, me], ag_send.at[a, k], ag_recv.at[a, me], target)
            copy.start()
            sends.append(copy)

    for a in range(pieces):
        for k in range(chips - 1, 0, -1):
            source = other(k) * 2 + core
            copy = remote(slots.at[a, source], slots.at[a, source], fw_send.at[a, k], ag_recv.at[a, source], partner)
            copy.wait_recv()
            copy.start()
            sends.append(copy)
        for k in range(chips):
            source = partner if k == 0 else other(k) * 2 + (1 - core)
            remote(slots.at[a, source], slots.at[a, source], fw_send.at[a, k], ag_recv.at[a, source], partner).wait_recv()
        for z in range(chips):
            both = jnp.concatenate([slots[a, 2 * z].astype(F32), slots[a, 2 * z + 1].astype(F32)], axis=0)
            hid_ref[2 * rows * z:2 * rows * (z + 1), a * span:(a + 1) * span] = both.astype(BF16)
        loads[a].wait()
        term = jnp.dot(
            hid_ref[:, a * span:(a + 1) * span], w_v[a * span:(a + 1) * span, :], preferred_element_type=F32
        )
        if a == 0:
            e_v[...] = term
        else:
            e_v[...] += term

    logits = e_v[...]
    target = jnp.transpose(jnp.broadcast_to(t_ref[...].astype(F32), (128, tokens)))[:, 0:1]
    columns = (me * width + lax.broadcasted_iota(jnp.int32, (tokens, width), 1)).astype(F32)
    hits = columns == target
    local_top = jnp.max(logits, axis=1, keepdims=True)
    expo = jnp.exp(logits - local_top)
    local_total = jnp.sum(expo, axis=1, keepdims=True)
    local_picked = jnp.sum(jnp.where(hits, logits, 0.0), axis=1, keepdims=True)
    e_v[...] = expo
    lane = lax.broadcasted_iota(jnp.int32, (tokens, 128), 1)
    packed = jnp.where(lane == 0, local_top, jnp.where(lane == 1, local_total, local_picked))
    stats[me] = jnp.transpose(packed)[0:8, :]
    for k in range(1, n):
        copy = remote(stats.at[me], stats.at[me], st_send.at[k], st_recv.at[me], lax.rem(me + k, n))
        copy.start()
        sends.append(copy)
    for b in range(blocks):
        turned_ref[b * tall:(b + 1) * tall, :] = jnp.transpose(hid_ref[:, b * tall:(b + 1) * tall])
    for k in range(1, n):
        source = lax.rem(me + k, n)
        remote(stats.at[source], stats.at[source], st_send.at[k], st_recv.at[source], source).wait_recv()

    top = stats[0, 0:1, :]
    for k in range(1, n):
        top = jnp.maximum(top, stats[k, 0:1, :])
    total = jnp.zeros_like(top)
    picked = jnp.zeros_like(top)
    for k in range(n):
        total += stats[k, 1:2, :] * jnp.exp(stats[k, 0:1, :] - top)
        picked += stats[k, 2:3, :]
    loss_ref[...] = jnp.sum(top + jnp.log(total) - picked, axis=1, keepdims=True) / tokens

    sub = lax.broadcasted_iota(jnp.int32, (128, tokens), 0)
    turned = jnp.transpose(jnp.where(sub == 0, top, total))
    factor = jnp.exp(local_top - turned[:, 0:1]) / turned[:, 1:2]
    grad = (e_v[...] * factor - hits.astype(F32)).astype(BF16)
    g_ref[...] = grad

    def pair_copy(j):
        return remote(part.at[j, 1 - core], xbuf.at[j], x_send.at[j], x_recv.at[j], partner)

    def group_copy(j, k):
        return remote(outb.at[j, other(k)], rbuf.at[j, chip], rs_send.at[j, k], rs_recv.at[j, chip], other(k) * 2 + core)

    def pass_on(j):
        pair_copy(j).wait_recv()
        for z in range(chips):
            outb[j, z] = (part[j, core, z] + xbuf[j, z]).astype(BF16)
        for k in range(1, chips):
            copy = group_copy(j, k)
            copy.start()
            sends.append(copy)

    for j in range(parts):
        term = lax.dot_general(
            g_ref[...], w_v[j * wide:(j + 1) * wide, :], (((1,), (1,)), ((), ())), preferred_element_type=F32
        )
        for z in range(chips):
            for half in range(2):
                at = (2 * z + half) * rows
                part[j, half, z] = term[at:at + rows, :]
        copy = pair_copy(j)
        copy.start()
        sends.append(copy)
        if j > 0:
            pass_on(j - 1)
    pass_on(parts - 1)
    for b in range(blocks):
        dw_ref[b * tall:(b + 1) * tall, :] = jnp.dot(
            turned_ref[b * tall:(b + 1) * tall, :], g_ref[...], preferred_element_type=F32
        ).astype(BF16)

    for j in range(parts):
        summed = part[j, core, chip] + xbuf[j, chip]
        for k in range(1, chips):
            source = other(k)
            remote(rbuf.at[j, source], rbuf.at[j, source], rs_send.at[j, k], rs_recv.at[j, source], source * 2 + core).wait_recv()
            summed += rbuf[j, source].astype(F32)
        dh_ref[:, j * wide:(j + 1) * wide] = summed.astype(BF16)

    for copy in sends:
        copy.wait_send()


def store_kernel(dw_v, dh_v, loss_v, dw_hbm, dh_hbm, loss_hbm, sem):
    copies = [pltpu.make_async_copy(dh_v, dh_hbm, sem.at[0]), pltpu.make_async_copy(loss_v, loss_hbm, sem.at[1])]
    count = sem.shape[0] - 2
    tall = dw_v.shape[0] // count
    for b in range(count):
        at = pl.ds(b * tall, tall)
        copies.append(pltpu.make_async_copy(dw_v.at[at, :], dw_hbm.at[at, :], sem.at[2 + b]))
    for copy in copies:
        copy.start()
    for copy in copies:
        copy.wait()


def body(n, hidden, weight, targets):
    rows, depth = hidden.shape
    width = weight.shape[1]
    tokens = rows * n
    chips = n // 2
    pieces = split(depth, 2, 256)
    parts = split(depth, 4, 256)
    span, wide = depth // pieces, depth // parts
    vmem = pl.BlockSpec(memory_space=pltpu.VMEM)
    dma = pltpu.SemaphoreType.DMA
    hbm = pl.BlockSpec(memory_space=pltpu.HBM)
    results = (
        jax.ShapeDtypeStruct((depth, width), BF16),
        jax.ShapeDtypeStruct((rows, depth), BF16),
        jax.ShapeDtypeStruct((1, 1), F32),
    )
    held = pl.pallas_call(
        functools.partial(loss_kernel, n),
        out_shape=results,
        in_specs=[hbm, hbm, hbm],
        out_specs=(vmem, vmem, vmem),
        scratch_shapes=[
            pltpu.VMEM((rows, depth), BF16),
            pltpu.VMEM((1, tokens), jnp.int32),
            pltpu.VMEM((tokens, depth), BF16),
            pltpu.VMEM((depth, tokens), BF16),
            pltpu.VMEM((tokens, width), BF16),
            pltpu.VMEM((depth, width), BF16),
            pltpu.VMEM((pieces, n, rows, span), BF16),
            pltpu.VMEM((tokens, width), F32),
            pltpu.VMEM((n, 8, tokens), F32),
            pltpu.VMEM((parts, 2, chips, rows, wide), F32),
            pltpu.VMEM((parts, chips, rows, wide), F32),
            pltpu.VMEM((parts, chips, rows, wide), BF16),
            pltpu.VMEM((parts, chips, rows, wide), BF16),
            dma((2,)),
            dma((pieces,)),
            dma((pieces, chips)),
            dma((pieces, chips)),
            dma((pieces, n)),
            dma((n,)),
            dma((n,)),
            dma((parts,)),
            dma((parts,)),
            dma((parts, chips)),
            dma((parts, chips)),
        ],
        compiler_params=pltpu.CompilerParams(
            collective_id=0, has_side_effects=True, vmem_limit_bytes=44 * 1024 * 1024
        ),
    )(hidden, weight, targets.reshape(1, tokens))
    d_weight, d_hidden, loss = pl.pallas_call(
        store_kernel,
        out_shape=results,
        in_specs=[vmem, vmem, vmem],
        out_specs=(hbm, hbm, hbm),
        scratch_shapes=[dma((6,))],
        compiler_params=pltpu.CompilerParams(vmem_limit_bytes=2 * 1024 * 1024),
    )(*held)
    return loss.reshape(1), d_hidden, d_weight


def solution(mesh):
    placed = (P(("dp", "vocab"), None), P(None, "vocab"), P("dp"))
    return jax.shard_map(
        functools.partial(body, mesh.shape["vocab"]),
        mesh=mesh,
        in_specs=placed,
        out_specs=(P("dp"), P(("dp", "vocab"), None), P("dp", "vocab")),
        check_vma=False,
    )
```

```python
import functools

import jax
import jax.numpy as jnp
from jax import lax
from jax.experimental import pallas as pl
from jax.experimental.pallas import tpu as pltpu
from jax.sharding import PartitionSpec as P

MESH = pl.DeviceIdType.MESH
F32 = jnp.float32
BF16 = jnp.bfloat16


def split(length, most, unit):
    for parts in range(most, 0, -1):
        if length % (parts * unit) == 0:
            return parts
    return 1


def remote(src, dst, send, recv, device):
    return pltpu.make_async_remote_copy(
        src_ref=src, dst_ref=dst, send_sem=send, recv_sem=recv, device_id={"vocab": device}, device_id_type=MESH
    )


def loss_kernel(
    n, h_hbm, w_hbm, t_hbm, dw_ref, dh_ref, loss_ref,
    h_ref, t_ref, hid_ref, turned_ref, g_ref, w_v, slots, e_v, stats, part, xbuf, outb, rbuf,
    in_sem, w_sem, ag_send, fw_send, ag_recv, st_send, st_recv, x_send, x_recv, rs_send, rs_recv,
):
    me = lax.axis_index("vocab")
    chips = n // 2
    chip, core = me // 2, me % 2
    partner = chip * 2 + (1 - core)
    rows, depth = h_ref.shape
    tokens, width = e_v.shape
    pieces, span = slots.shape[0], slots.shape[3]
    parts, wide = part.shape[0], part.shape[4]
    blocks = split(depth, 6, 256)
    tall = depth // blocks

    above = chips - 1 - chip

    def other(k):
        up = (above - k + chips) // chips
        return up * (chips - k) + (1 - up) * (k - 1 - above)

    takes = [pltpu.make_async_copy(h_hbm, h_ref, in_sem.at[0]), pltpu.make_async_copy(t_hbm, t_ref, in_sem.at[1])]
    for take in takes:
        take.start()
    loads = [
        pltpu.make_async_copy(w_hbm.at[pl.ds(a * span, span), :], w_v.at[pl.ds(a * span, span), :], w_sem.at[a])
        for a in range(pieces)
    ]
    for load in loads:
        load.start()

    barrier = pltpu.get_barrier_semaphore()
    for k in range(1, n):
        pl.semaphore_signal(barrier, inc=1, device_id={"vocab": lax.rem(me + k, n)}, device_id_type=MESH)
    for take in takes:
        take.wait()
    for a in range(pieces):
        slots[a, me] = h_ref[:, a * span:(a + 1) * span]
    pl.semaphore_wait(barrier, n - 1)

    sends = []
    for a in range(pieces):
        own = h_ref.at[:, pl.ds(a * span, span)]
        for k in range(chips):
            target = partner if k == 0 else other(k) * 2 + core
            copy = remote(own, slots.at[a, me], ag_send.at[a, k], ag_recv.at[a, me], target)
            copy.start()
            sends.append(copy)

    for a in range(pieces):
        for k in range(chips - 1, 0, -1):
            source = other(k) * 2 + core
            copy = remote(slots.at[a, source], slots.at[a, source], fw_send.at[a, k], ag_recv.at[a, source], partner)
            copy.wait_recv()
            copy.start()
            sends.append(copy)
        for k in range(chips):
            source = partner if k == 0 else other(k) * 2 + (1 - core)
            remote(slots.at[a, source], slots.at[a, source], fw_send.at[a, k], ag_recv.at[a, source], partner).wait_recv()
        for z in range(chips):
            both = jnp.concatenate([slots[a, 2 * z].astype(F32), slots[a, 2 * z + 1].astype(F32)], axis=0)
            hid_ref[2 * rows * z:2 * rows * (z + 1), a * span:(a + 1) * span] = both.astype(BF16)
        loads[a].wait()
        term = jnp.dot(
            hid_ref[:, a * span:(a + 1) * span], w_v[a * span:(a + 1) * span, :], preferred_element_type=F32
        )
        if a == 0:
            e_v[...] = term
        else:
            e_v[...] += term

    logits = e_v[...]
    target = jnp.transpose(jnp.broadcast_to(t_ref[...].astype(F32), (128, tokens)))[:, 0:1]
    columns = (me * width + lax.broadcasted_iota(jnp.int32, (tokens, width), 1)).astype(F32)
    hits = columns == target
    local_top = jnp.max(logits, axis=1, keepdims=True)
    expo = jnp.exp(logits - local_top)
    local_total = jnp.sum(expo, axis=1, keepdims=True)
    local_picked = jnp.sum(jnp.where(hits, logits, 0.0), axis=1, keepdims=True)
    e_v[...] = expo
    lane = lax.broadcasted_iota(jnp.int32, (tokens, 128), 1)
    packed = jnp.where(lane == 0, local_top, jnp.where(lane == 1, local_total, local_picked))
    stats[me] = jnp.transpose(packed)[0:8, :]
    for k in range(1, n):
        copy = remote(stats.at[me], stats.at[me], st_send.at[k], st_recv.at[me], lax.rem(me + k, n))
        copy.start()
        sends.append(copy)
    for b in range(blocks):
        turned_ref[b * tall:(b + 1) * tall, :] = jnp.transpose(hid_ref[:, b * tall:(b + 1) * tall])
    for k in range(1, n):
        source = lax.rem(me + k, n)
        remote(stats.at[source], stats.at[source], st_send.at[k], st_recv.at[source], source).wait_recv()

    top = stats[0, 0:1, :]
    for k in range(1, n):
        top = jnp.maximum(top, stats[k, 0:1, :])
    total = jnp.zeros_like(top)
    picked = jnp.zeros_like(top)
    for k in range(n):
        total += stats[k, 1:2, :] * jnp.exp(stats[k, 0:1, :] - top)
        picked += stats[k, 2:3, :]
    loss_ref[...] = jnp.broadcast_to(jnp.sum(top + jnp.log(total) - picked, axis=1, keepdims=True) / tokens, loss_ref.shape)

    sub = lax.broadcasted_iota(jnp.int32, (128, tokens), 0)
    turned = jnp.transpose(jnp.where(sub == 0, top, total))
    factor = jnp.exp(local_top - turned[:, 0:1]) / turned[:, 1:2]
    grad = (e_v[...] * factor - hits.astype(F32)).astype(BF16)
    g_ref[...] = grad

    def pair_copy(j):
        return remote(part.at[j, 1 - core], xbuf.at[j], x_send.at[j], x_recv.at[j], partner)

    def group_copy(j, k):
        return remote(outb.at[j, other(k)], rbuf.at[j, chip], rs_send.at[j, k], rs_recv.at[j, chip], other(k) * 2 + core)

    def pass_on(j):
        pair_copy(j).wait_recv()
        for z in range(chips):
            outb[j, z] = (part[j, core, z] + xbuf[j, z]).astype(BF16)
        for k in range(1, chips):
            copy = group_copy(j, k)
            copy.start()
            sends.append(copy)

    for j in range(parts):
        term = lax.dot_general(
            g_ref[...], w_v[j * wide:(j + 1) * wide, :], (((1,), (1,)), ((), ())), preferred_element_type=F32
        )
        for z in range(chips):
            for half in range(2):
                at = (2 * z + half) * rows
                part[j, half, z] = term[at:at + rows, :]
        copy = pair_copy(j)
        copy.start()
        sends.append(copy)
        if j > 0:
            pass_on(j - 1)
    pass_on(parts - 1)
    for b in range(blocks):
        dw_ref[b * tall:(b + 1) * tall, :] = jnp.dot(
            turned_ref[b * tall:(b + 1) * tall, :], g_ref[...], preferred_element_type=F32
        ).astype(BF16)

    for j in range(parts):
        summed = part[j, core, chip] + xbuf[j, chip]
        for k in range(1, chips):
            source = other(k)
            remote(rbuf.at[j, source], rbuf.at[j, source], rs_send.at[j, k], rs_recv.at[j, source], source * 2 + core).wait_recv()
            summed += rbuf[j, source].astype(F32)
        dh_ref[:, j * wide:(j + 1) * wide] = summed.astype(BF16)

    for copy in sends:
        copy.wait_send()


def store_kernel(dw_v, dh_v, loss_v, dw_hbm, dh_hbm, loss_hbm, one_v, sem):
    one_v[...] = loss_v[0:1, 0:1]
    copies = []
    count = sem.shape[0] - 2
    tall = dw_v.shape[0] // count
    for b in range(count):
        at = pl.ds(b * tall, tall)
        copies.append(pltpu.make_async_copy(dw_v.at[at, :], dw_hbm.at[at, :], sem.at[2 + b]))
    copies.append(pltpu.make_async_copy(dh_v, dh_hbm, sem.at[0]))
    copies.append(pltpu.make_async_copy(one_v, loss_hbm, sem.at[1]))
    for copy in copies:
        copy.start()
    for copy in copies:
        copy.wait()


def body(n, hidden, weight, targets):
    rows, depth = hidden.shape
    width = weight.shape[1]
    tokens = rows * n
    chips = n // 2
    pieces = split(depth, 4, 256)
    parts = split(depth, 4, 256)
    span, wide = depth // pieces, depth // parts
    vmem = pl.BlockSpec(memory_space=pltpu.VMEM)
    dma = pltpu.SemaphoreType.DMA
    hbm = pl.BlockSpec(memory_space=pltpu.HBM)
    shared = (jax.ShapeDtypeStruct((depth, width), BF16), jax.ShapeDtypeStruct((rows, depth), BF16))
    tile = jax.ShapeDtypeStruct((8, 128), F32)
    held = pl.pallas_call(
        functools.partial(loss_kernel, n),
        out_shape=(*shared, tile),
        in_specs=[hbm, hbm, hbm],
        out_specs=(vmem, vmem, vmem),
        scratch_shapes=[
            pltpu.VMEM((rows, depth), BF16),
            pltpu.VMEM((1, tokens), jnp.int32),
            pltpu.VMEM((tokens, depth), BF16),
            pltpu.VMEM((depth, tokens), BF16),
            pltpu.VMEM((tokens, width), BF16),
            pltpu.VMEM((depth, width), BF16),
            pltpu.VMEM((pieces, n, rows, span), BF16),
            pltpu.VMEM((tokens, width), F32),
            pltpu.VMEM((n, 8, tokens), F32),
            pltpu.VMEM((parts, 2, chips, rows, wide), F32),
            pltpu.VMEM((parts, chips, rows, wide), F32),
            pltpu.VMEM((parts, chips, rows, wide), BF16),
            pltpu.VMEM((parts, chips, rows, wide), BF16),
            dma((2,)),
            dma((pieces,)),
            dma((pieces, chips)),
            dma((pieces, chips)),
            dma((pieces, n)),
            dma((n,)),
            dma((n,)),
            dma((parts,)),
            dma((parts,)),
            dma((parts, chips)),
            dma((parts, chips)),
        ],
        compiler_params=pltpu.CompilerParams(
            collective_id=0, has_side_effects=True, vmem_limit_bytes=45 * 1024 * 1024
        ),
    )(hidden, weight, targets.reshape(1, tokens))
    d_weight, d_hidden, loss = pl.pallas_call(
        store_kernel,
        out_shape=(*shared, jax.ShapeDtypeStruct((1, 1), F32)),
        in_specs=[vmem, vmem, vmem],
        out_specs=(hbm, hbm, hbm),
        scratch_shapes=[pltpu.VMEM((1, 1), F32), dma((2 + split(depth, 12, 16),))],
        compiler_params=pltpu.CompilerParams(vmem_limit_bytes=2 * 1024 * 1024),
    )(*held)
    return loss.reshape(1), d_hidden, d_weight


def solution(mesh):
    placed = (P(("dp", "vocab"), None), P(None, "vocab"), P("dp"))
    return jax.shard_map(
        functools.partial(body, mesh.shape["vocab"]),
        mesh=mesh,
        in_specs=placed,
        out_specs=(P("dp"), P(("dp", "vocab"), None), P("dp", "vocab")),
        check_vma=False,
    )
```

```python
import functools

import jax
import jax.numpy as jnp
from jax import lax
from jax.experimental import pallas as pl
from jax.experimental.pallas import tpu as pltpu
from jax.sharding import PartitionSpec as P

MESH = pl.DeviceIdType.MESH
F32 = jnp.float32
BF16 = jnp.bfloat16


def split(length, most, unit):
    for parts in range(most, 0, -1):
        if length % (parts * unit) == 0:
            return parts
    return 1


def remote(src, dst, send, recv, device):
    return pltpu.make_async_remote_copy(
        src_ref=src, dst_ref=dst, send_sem=send, recv_sem=recv, device_id={"vocab": device}, device_id_type=MESH
    )


def loss_kernel(
    n, h_hbm, w_hbm, t_hbm, dw_ref, dh_ref, loss_ref,
    h_ref, t_ref, aim_ref, hid_ref, turned_ref, g_ref, w_v, slots, e_v, stats, part, xbuf, outb, rbuf,
    in_sem, w_sem, ag_send, fw_send, ag_recv, st_send, st_recv, x_send, x_recv, rs_send, rs_recv,
):
    me = lax.axis_index("vocab")
    chips = n // 2
    chip, core = me // 2, me % 2
    partner = chip * 2 + (1 - core)
    rows, depth = h_ref.shape
    tokens, width = e_v.shape
    pieces, span = slots.shape[0], slots.shape[3]
    parts, wide = part.shape[0], part.shape[4]
    blocks = split(depth, 6, 256)
    tall = depth // blocks

    above = chips - 1 - chip

    def other(k):
        up = (above - k + chips) // chips
        return up * (chips - k) + (1 - up) * (k - 1 - above)

    takes = [pltpu.make_async_copy(h_hbm, h_ref, in_sem.at[0]), pltpu.make_async_copy(t_hbm, t_ref, in_sem.at[1])]
    for take in takes:
        take.start()
    loads = [
        pltpu.make_async_copy(w_hbm.at[pl.ds(a * span, span), :], w_v.at[pl.ds(a * span, span), :], w_sem.at[a])
        for a in range(pieces)
    ]
    for load in loads:
        load.start()

    barrier = pltpu.get_barrier_semaphore()
    for k in range(1, n):
        pl.semaphore_signal(barrier, inc=1, device_id={"vocab": lax.rem(me + k, n)}, device_id_type=MESH)
    for take in takes:
        take.wait()
    for a in range(pieces):
        slots[a, me] = h_ref[:, a * span:(a + 1) * span]
    aim_ref[...] = jnp.transpose(jnp.broadcast_to((t_ref[...] - me * width).astype(F32), (128, tokens)))
    pl.semaphore_wait(barrier, n - 1)

    sends = []
    for a in range(pieces):
        own = h_ref.at[:, pl.ds(a * span, span)]
        for k in range(chips):
            target = partner if k == 0 else other(k) * 2 + core
            copy = remote(own, slots.at[a, me], ag_send.at[a, k], ag_recv.at[a, me], target)
            copy.start()
            sends.append(copy)

    for a in range(pieces):
        for k in range(chips - 1, 0, -1):
            source = other(k) * 2 + core
            copy = remote(slots.at[a, source], slots.at[a, source], fw_send.at[a, k], ag_recv.at[a, source], partner)
            copy.wait_recv()
            copy.start()
            sends.append(copy)
        for k in range(chips):
            source = partner if k == 0 else other(k) * 2 + (1 - core)
            remote(slots.at[a, source], slots.at[a, source], fw_send.at[a, k], ag_recv.at[a, source], partner).wait_recv()
        for z in range(chips):
            both = jnp.concatenate([slots[a, 2 * z].astype(F32), slots[a, 2 * z + 1].astype(F32)], axis=0)
            hid_ref[2 * rows * z:2 * rows * (z + 1), a * span:(a + 1) * span] = both.astype(BF16)
        loads[a].wait()
        term = jnp.dot(
            hid_ref[:, a * span:(a + 1) * span], w_v[a * span:(a + 1) * span, :], preferred_element_type=F32
        )
        if a == 0:
            e_v[...] = term
        else:
            e_v[...] += term

    logits = e_v[...]
    hits = lax.broadcasted_iota(jnp.int32, (tokens, width), 1).astype(F32) == aim_ref[:, 0:1]
    local_top = jnp.max(logits, axis=1, keepdims=True)
    expo = jnp.exp(logits - local_top)
    local_total = jnp.sum(expo, axis=1, keepdims=True)
    local_picked = jnp.sum(jnp.where(hits, logits, 0.0), axis=1, keepdims=True)
    e_v[...] = expo
    lane = lax.broadcasted_iota(jnp.int32, (tokens, 128), 1)
    packed = jnp.where(lane == 0, local_top, jnp.where(lane == 1, local_total, local_picked))
    stats[me] = jnp.transpose(packed)[0:8, :]
    for k in range(1, n):
        copy = remote(stats.at[me], stats.at[me], st_send.at[k], st_recv.at[me], lax.rem(me + k, n))
        copy.start()
        sends.append(copy)
    for b in range(blocks):
        turned_ref[b * tall:(b + 1) * tall, :] = jnp.transpose(hid_ref[:, b * tall:(b + 1) * tall])
    for k in range(1, n):
        source = lax.rem(me + k, n)
        remote(stats.at[source], stats.at[source], st_send.at[k], st_recv.at[source], source).wait_recv()

    top = stats[0, 0:1, :]
    for k in range(1, n):
        top = jnp.maximum(top, stats[k, 0:1, :])
    total = jnp.zeros_like(top)
    picked = jnp.zeros_like(top)
    for k in range(n):
        total += stats[k, 1:2, :] * jnp.exp(stats[k, 0:1, :] - top)
        picked += stats[k, 2:3, :]
    loss_ref[...] = jnp.broadcast_to(jnp.sum(top + jnp.log(total) - picked, axis=1, keepdims=True) / tokens, loss_ref.shape)

    sub = lax.broadcasted_iota(jnp.int32, (128, tokens), 0)
    turned = jnp.transpose(jnp.where(sub == 0, top, total))
    factor = jnp.exp(local_top - turned[:, 0:1]) / turned[:, 1:2]
    grad = (e_v[...] * factor - hits.astype(F32)).astype(BF16)
    g_ref[...] = grad

    def pair_copy(j):
        return remote(part.at[j, 1 - core], xbuf.at[j], x_send.at[j], x_recv.at[j], partner)

    def group_copy(j, k):
        return remote(outb.at[j, other(k)], rbuf.at[j, chip], rs_send.at[j, k], rs_recv.at[j, chip], other(k) * 2 + core)

    def pass_on(j):
        pair_copy(j).wait_recv()
        for z in range(chips):
            outb[j, z] = (part[j, core, z] + xbuf[j, z]).astype(BF16)
        for k in range(1, chips):
            copy = group_copy(j, k)
            copy.start()
            sends.append(copy)

    for j in range(parts):
        term = lax.dot_general(
            g_ref[...], w_v[j * wide:(j + 1) * wide, :], (((1,), (1,)), ((), ())), preferred_element_type=F32
        )
        for z in range(chips):
            for half in range(2):
                at = (2 * z + half) * rows
                part[j, half, z] = term[at:at + rows, :]
        copy = pair_copy(j)
        copy.start()
        sends.append(copy)
        if j > 0:
            pass_on(j - 1)
    pass_on(parts - 1)
    for b in range(blocks):
        dw_ref[b * tall:(b + 1) * tall, :] = jnp.dot(
            turned_ref[b * tall:(b + 1) * tall, :], g_ref[...], preferred_element_type=F32
        ).astype(BF16)

    for j in range(parts):
        summed = part[j, core, chip] + xbuf[j, chip]
        for k in range(1, chips):
            source = other(k)
            remote(rbuf.at[j, source], rbuf.at[j, source], rs_send.at[j, k], rs_recv.at[j, source], source * 2 + core).wait_recv()
            summed += rbuf[j, source].astype(F32)
        dh_ref[:, j * wide:(j + 1) * wide] = summed.astype(BF16)

    for copy in sends:
        copy.wait_send()


def store_kernel(dw_v, dh_v, loss_v, dw_hbm, dh_hbm, loss_hbm, one_v, sem):
    one_v[...] = loss_v[0:1, 0:1]
    copies = []
    count = sem.shape[0] - 2
    tall = dw_v.shape[0] // count
    for b in range(count):
        at = pl.ds(b * tall, tall)
        copies.append(pltpu.make_async_copy(dw_v.at[at, :], dw_hbm.at[at, :], sem.at[2 + b]))
    copies.append(pltpu.make_async_copy(dh_v, dh_hbm, sem.at[0]))
    copies.append(pltpu.make_async_copy(one_v, loss_hbm, sem.at[1]))
    for copy in copies:
        copy.start()
    for copy in copies:
        copy.wait()


def body(n, hidden, weight, targets):
    rows, depth = hidden.shape
    width = weight.shape[1]
    tokens = rows * n
    chips = n // 2
    pieces = split(depth, 2, 256)
    parts = split(depth, 6, 256)
    span, wide = depth // pieces, depth // parts
    vmem = pl.BlockSpec(memory_space=pltpu.VMEM)
    dma = pltpu.SemaphoreType.DMA
    hbm = pl.BlockSpec(memory_space=pltpu.HBM)
    shared = (jax.ShapeDtypeStruct((depth, width), BF16), jax.ShapeDtypeStruct((rows, depth), BF16))
    tile = jax.ShapeDtypeStruct((8, 128), F32)
    held = pl.pallas_call(
        functools.partial(loss_kernel, n),
        out_shape=(*shared, tile),
        in_specs=[hbm, hbm, hbm],
        out_specs=(vmem, vmem, vmem),
        scratch_shapes=[
            pltpu.VMEM((rows, depth), BF16),
            pltpu.VMEM((1, tokens), jnp.int32),
            pltpu.VMEM((tokens, 128), F32),
            pltpu.VMEM((tokens, depth), BF16),
            pltpu.VMEM((depth, tokens), BF16),
            pltpu.VMEM((tokens, width), BF16),
            pltpu.VMEM((depth, width), BF16),
            pltpu.VMEM((pieces, n, rows, span), BF16),
            pltpu.VMEM((tokens, width), F32),
            pltpu.VMEM((n, 8, tokens), F32),
            pltpu.VMEM((parts, 2, chips, rows, wide), F32),
            pltpu.VMEM((parts, chips, rows, wide), F32),
            pltpu.VMEM((parts, chips, rows, wide), BF16),
            pltpu.VMEM((parts, chips, rows, wide), BF16),
            dma((2,)),
            dma((pieces,)),
            dma((pieces, chips)),
            dma((pieces, chips)),
            dma((pieces, n)),
            dma((n,)),
            dma((n,)),
            dma((parts,)),
            dma((parts,)),
            dma((parts, chips)),
            dma((parts, chips)),
        ],
        compiler_params=pltpu.CompilerParams(
            collective_id=0, has_side_effects=True, vmem_limit_bytes=45 * 1024 * 1024
        ),
    )(hidden, weight, targets.reshape(1, tokens))
    d_weight, d_hidden, loss = pl.pallas_call(
        store_kernel,
        out_shape=(*shared, jax.ShapeDtypeStruct((1, 1), F32)),
        in_specs=[vmem, vmem, vmem],
        out_specs=(hbm, hbm, hbm),
        scratch_shapes=[pltpu.VMEM((1, 1), F32), dma((2 + split(depth, 12, 16),))],
        compiler_params=pltpu.CompilerParams(vmem_limit_bytes=2 * 1024 * 1024),
    )(*held)
    return loss.reshape(1), d_hidden, d_weight


def solution(mesh):
    placed = (P(("dp", "vocab"), None), P(None, "vocab"), P("dp"))
    return jax.shard_map(
        functools.partial(body, mesh.shape["vocab"]),
        mesh=mesh,
        in_specs=placed,
        out_specs=(P("dp"), P(("dp", "vocab"), None), P("dp", "vocab")),
        check_vma=False,
    )
```
